32 devices in a mesh: gx: 2 (over x), gy: 4 (over z), gz: 4 (over y, core).
Axes of the slice: x: 2, y: 2, z: 4, core: 2. Of those that a mesh axis runs over, the one named last changes fastest.
Arguments:
- density: float32 [32, 64, 512], P('gx', 'gy', 'gz'), may hold values from 0.005 to 0.6, as said below
- coupling: float32 [14, 14], replicated, may hold values from -0.3 to 1.5, as said below
Outputs:
- potentials: float32 [14, 32, 64, 512], P(None, 'gx', 'gy', 'gz')
The draws below stay inside these ranges and needn't reach their ends.
Inputs may be any that keep to these rules, and one draw needn't show every extreme that they name: Positive density. `coupling`: symmetric.
All inputs are finite; a program needn't handle non-finite values.
Results may differ from the reference program's by a relative error of at most 0.0003.
Values sent between devices are 32-bit elements; how exact they have to be, the bound alone decides.
A program may use at most 128 MiB of HBM per device.

```python
import math
import jax
import jax.numpy as jnp
from jax import lax

NQ = 14
NX = 32
NY = 64
NZ = 512


def draw_density(key, part):
    rough_key = jax.random.fold_in(key, 11)
    along_x = jnp.arange(NX, dtype=jnp.float32) / NX
    along_y = jnp.arange(NY, dtype=jnp.float32) / NY
    along_z = jnp.arange(NZ, dtype=jnp.float32) / NZ
    envelope = (along_x[:, None, None] + 0.7 * along_y[None, :, None] + 0.5 * along_z[None, None, :]) / 2.2
    roughness = jax.random.uniform(rough_key, (NX, NY, NZ), jnp.float32, -1.0, 1.0)
    return 0.01 * jnp.exp(math.log(40.0) * envelope) * (1.0 + 0.5 * roughness)


def draw_coupling(key, part):
    base_key = jax.random.fold_in(key, 23)
    diag_key = jax.random.fold_in(key, 29)
    entries = jax.random.uniform(base_key, (NQ, NQ), jnp.float32, -1.0, 1.0)
    diagonal = jax.random.uniform(diag_key, (NQ,), jnp.float32, 0.8, 1.2)
    return 0.15 * (entries + entries.T) + jnp.diag(diagonal)


def setup_inputs(seed: int = 0) -> dict:
    key_of = jax.random.split(jax.random.key(seed), 3)
    density = draw_density(jax.random.fold_in(key_of[2], 71), 0)
    coupling = draw_coupling(jax.random.fold_in(key_of[2], 71), 0)
    return dict(density=density, coupling=coupling)


zab_ratio = 0.8491 / 9.0
q_cut = 5.0
mesh_step = 0.07
range_factor = 1.0
local_weight = 0.25
spline_root = math.sqrt(3.0) - 2.0
highest = lax.Precision.HIGHEST

def gradient_squared(density):
    summed = jnp.zeros_like(density)
    for dim_index in range(3):
        nearer = jnp.roll(density, -1, dim_index) - jnp.roll(density, 1, dim_index)
        farther = jnp.roll(density, -2, dim_index) - jnp.roll(density, 2, dim_index)
        gradient = (8.0 * nearer - farther) / 12.0
        summed = summed + gradient * gradient
    return summed

def saturated_wavevector(density, grad_sq):
    fermi_k = jnp.cbrt(3.0 * math.pi * math.pi * density)
    reduced = grad_sq / (4.0 * fermi_k * fermi_k * density * density)
    raw_q = fermi_k * (1.0 + zab_ratio * reduced)
    scaled = raw_q / q_cut
    powered = scaled
    series = jnp.zeros_like(scaled)
    for term_order in range(1, 13):
        series = series + powered / term_order
        powered = powered * scaled
    return q_cut * (1.0 - jnp.exp(-series))

def spline_weights(q_zero, q_top, qpoints):
    position = jnp.maximum(qpoints - 1.0 + jnp.log(q_zero / q_top) / mesh_step, 0.0)
    knot_ids = jnp.arange(-1, qpoints + 1, dtype=jnp.int32)
    offset = jnp.abs(position[None, :] - knot_ids.astype(jnp.float32)[:, None])
    bspline = (jnp.maximum(2.0 - offset, 0.0) ** 3 - 4.0 * jnp.maximum(1.0 - offset, 0.0) ** 3) / 6.0
    q_nodes = jnp.arange(qpoints, dtype=jnp.int32)
    distance = jnp.abs(knot_ids[:, None] - q_nodes[None, :])
    parity = (1 - 2 * (distance % 2)).astype(jnp.float32)
    matrix = math.sqrt(3.0) * parity * jnp.exp(distance.astype(jnp.float32) * math.log(-spline_root))
    return jnp.dot(matrix.T, bspline, precision=highest)

def wave_squared(wave_ids, length):
    folded = jnp.where(2 * wave_ids < length, wave_ids, wave_ids - length)
    wavenum = 2.0 * math.pi / length * folded.astype(jnp.float32)
    return wavenum * wavenum

def reference(density, coupling):
    qpoints = coupling.shape[0]
    grad_sq = gradient_squared(density)
    q_zero = saturated_wavevector(density, grad_sq)
    q_top = jnp.max(q_zero)

    def one_plane(x_plane):
        dens_plane, q_plane = x_plane
        weights = spline_weights(q_plane.reshape(-1), q_top, qpoints)
        return weights * dens_plane.reshape(1, -1)
    thetas = lax.map(one_plane, (density, q_zero))
    thetas = jnp.transpose(thetas, (1, 0, 2)).reshape(qpoints, NX, NY, NZ)
    spectra = jnp.fft.fftn(thetas, axes=(1, 2, 3))
    k_squared = wave_squared(jnp.arange(NX, dtype=jnp.int32), NX)[:, None, None] + wave_squared(jnp.arange(NY, dtype=jnp.int32), NY)[None, :, None] + wave_squared(jnp.arange(NZ, dtype=jnp.int32), NZ)[None, None, :]
    q_nodes = jnp.arange(qpoints, dtype=jnp.int32)
    q_mesh = q_top * jnp.exp(-mesh_step * (qpoints - 1 - q_nodes).astype(jnp.float32))
    masses = range_factor * q_mesh[:, None] * q_mesh[None, :]

    def potential(target):

        def add_source(source, summed):
            factor = coupling[target, source] * (local_weight + masses[target, source] / (k_squared + masses[target, source]))
            return summed + factor * spectra[source]
        summed = lax.fori_loop(0, qpoints, add_source, jnp.zeros_like(spectra[0]))
        return jnp.real(jnp.fft.ifftn(summed)).astype(jnp.float32)
    return lax.map(potential, q_nodes)
```

```python
import math

import jax
import jax.numpy as jnp
import ml_dtypes
import numpy as np
from jax import lax
from jax.experimental import pallas as pl
from jax.experimental.pallas import tpu as pltpu
from jax.sharding import PartitionSpec as P

zab_ratio = 0.8491 / 9.0
q_cut = 5.0
mesh_step = 0.07
range_factor = 1.0
local_weight = 0.25
spline_root = math.sqrt(3.0) - 2.0
vmem_bytes = 60 * 1024 * 1024


def hartley(length):
    ids = np.arange(length)
    angles = 2.0 * np.pi / length * (ids[:, None] * ids[None, :] % length)
    return np.cos(angles) + np.sin(angles)


def split_table(table):
    table = np.asarray(table, np.float32)
    high = table.astype(ml_dtypes.bfloat16)
    low = (table - high.astype(np.float32)).astype(ml_dtypes.bfloat16)
    return jnp.asarray(high), jnp.asarray(low)


def split_value(value):
    high = value.astype(jnp.bfloat16)
    low = (value - high.astype(jnp.float32)).astype(jnp.bfloat16)
    return high, low


def mul(left, right):
    def dot(a, b):
        return jnp.dot(a, b, preferred_element_type=jnp.float32)

    return dot(left[0], right[0]) + (dot(left[0], right[1]) + dot(left[1], right[0]))


def wave_squared(length):
    ids = np.arange(length)
    folded = np.where(2 * ids < length, ids, ids - length)
    wavenum = (2.0 * np.pi / length) * folded
    return (wavenum * wavenum).astype(np.float32)


def spline_matrix(qpoints):
    knots = np.arange(-1, qpoints + 1)
    nodes = np.arange(qpoints)
    return math.sqrt(3.0) * spline_root ** np.abs(knots[None, :] - nodes[:, None]).astype(np.float64)


def saturated_wavevector(density, grad_sq):
    fermi_k = jnp.cbrt(3.0 * math.pi * math.pi * density)
    reduced = grad_sq / (4.0 * fermi_k * fermi_k * density * density)
    raw_q = fermi_k * (1.0 + zab_ratio * reduced)
    scaled = raw_q / q_cut
    powered = scaled
    series = jnp.zeros_like(scaled)
    for term_order in range(1, 13):
        series = series + powered / term_order
        powered = powered * scaled
    return q_cut * (1.0 - jnp.exp(-series))


def with_halo(cells, axis, count, dim):
    size = cells.shape[dim]
    head = lax.slice_in_dim(cells, 0, 2, axis=dim)
    tail = lax.slice_in_dim(cells, size - 2, size, axis=dim)
    before = lax.ppermute(tail, axis, [(i, (i + 1) % count) for i in range(count)])
    after = lax.ppermute(head, axis, [((i + 1) % count, i) for i in range(count)])
    return jnp.concatenate([before, cells, after], axis=dim)


def slope_squared(padded, dim):
    size = padded.shape[dim] - 4

    def at(offset):
        return lax.slice_in_dim(padded, 2 + offset, 2 + offset + size, axis=dim)

    slope = (8.0 * (at(1) - at(-1)) - (at(2) - at(-2))) / 12.0
    return slope * slope


def global_max(value, axes):
    for axis in axes:
        count = lax.axis_size(axis)
        shifted = [
            lax.ppermute(value, axis, [(i, (i + step) % count) for i in range(count)])
            for step in range(1, count)
        ]
        for other in shifted:
            value = jnp.maximum(value, other)
    return value


def theta_kernel(qpoints, groups, weights, dens_ref, pos_ref, high_ref, low_ref, out_ref, spline_ref, theta_ref):
    rows, full = dens_ref.shape
    part = full // groups
    position = pos_ref[...]
    for knot in range(qpoints + 2):
        offset = jnp.abs(position - float(knot - 1))
        outer = jnp.maximum(2.0 - offset, 0.0)
        inner = jnp.maximum(1.0 - offset, 0.0)
        spline_ref[knot] = (outer * outer * outer - 4.0 * (inner * inner * inner)) / 6.0
    for row in range(0, rows, 8):
        picked = pl.ds(row, 8)
        density = dens_ref[picked, :]
        for node in range(qpoints):
            total = weights[node][0] * spline_ref[0, picked, :]
            for knot in range(1, qpoints + 2):
                total = total + weights[node][knot] * spline_ref[knot, picked, :]
            theta_ref[pl.ds(node * rows + row, 8), :] = total * density
    table = (high_ref[...], low_ref[...])

    def transform(step, carry):
        chunk = theta_ref[pl.ds(pl.multiple_of(step * 2 * rows, 8), 2 * rows), :]
        product = mul(split_value(chunk), table)
        for group in range(groups):
            piece = product[:, group * part : (group + 1) * part]
            out_ref[group, pl.ds(2 * step, 2)] = piece.reshape(2, rows, part)
        return carry

    lax.fori_loop(0, qpoints // 2, transform, 0)


def line_kernel(high_ref, low_ref, in_ref, out_ref):
    groups_in, fields, rows_in, lanes = in_ref.shape
    groups_out, _, rows_out, _ = out_ref.shape
    table = (high_ref[...], low_ref[...])
    for field in range(fields):
        data = in_ref[:, field].reshape(groups_in * rows_in, lanes)
        product = mul(table, split_value(data))
        out_ref[:, field] = product.reshape(groups_out, rows_out, lanes)


def product_kernel(coup_ref, mass_ref, high_ref, low_ref, wave_ref, in_ref, out_ref, spec_ref):
    groups, qpoints, rows, lanes = in_ref.shape
    total_rows = groups * rows
    table = (high_ref[...], low_ref[...])
    for field in range(qpoints):
        data = in_ref[:, field].reshape(total_rows, lanes)
        spec_ref[field] = mul(table, split_value(data))

    def couple(step, carry):
        picked = pl.ds(pl.multiple_of(step * 8, 8), 8)
        waves = wave_ref[picked, :]
        spectra = [spec_ref[field, picked, :] for field in range(qpoints)]
        sums = [None] * qpoints
        for level in range(2 * qpoints - 1):
            mass = mass_ref[level]
            factor = local_weight + mass / (waves + mass)
            for target in range(max(0, level - qpoints + 1), min(qpoints, level + 1)):
                source = level - target
                term = (coup_ref[target, source] * factor) * spectra[source]
                sums[target] = term if sums[target] is None else sums[target] + term
        for field in range(qpoints):
            spec_ref[field, picked, :] = sums[field]
        return carry

    lax.fori_loop(0, total_rows // 8, couple, 0)
    for field in range(qpoints):
        product = mul(table, split_value(spec_ref[field]))
        out_ref[:, field] = product.reshape(groups, rows, lanes)


def inverse_z_kernel(high_ref, low_ref, in_ref, out_ref):
    groups, fields, rows, part = in_ref.shape
    table = (high_ref[...], low_ref[...])

    def transform(step, carry):
        picked = pl.ds(2 * step, 2)
        pieces = [in_ref[group, picked].reshape(2 * rows, part) for group in range(groups)]
        product = mul(split_value(jnp.concatenate(pieces, axis=1)), table)
        groups_out, _, _, part_out = out_ref.shape
        for group in range(groups_out):
            piece = product[:, group * part_out : (group + 1) * part_out]
            out_ref[group, picked] = piece.reshape(2, rows, part_out)
        return carry

    lax.fori_loop(0, fields // 2, transform, 0)


def call(kernel, shape, specs, scratch=()):
    return pl.pallas_call(
        kernel,
        out_shape=jax.ShapeDtypeStruct(shape, jnp.float32),
        in_specs=[pl.BlockSpec(memory_space=space) for space in specs],
        out_specs=pl.BlockSpec(memory_space=pltpu.VMEM),
        scratch_shapes=list(scratch),
        compiler_params=pltpu.CompilerParams(vmem_limit_bytes=vmem_bytes),
    )


def exchange(value, axes):
    return lax.all_to_all(value, axes, split_axis=0, concat_axis=0, tiled=True)


def body(density, coupling):
    size_x, size_y, size_z = density.shape
    qpoints = coupling.shape[0]
    groups_x, groups_y, groups_z = (lax.axis_size("gx"), lax.axis_size("gy"), lax.axis_size("gz"))
    full_x, full_y, full_z = (size_x * groups_x, size_y * groups_y, size_z * groups_z)
    slab = size_x // groups_z
    groups_xz = groups_x * groups_z
    part_y = full_y // groups_xz
    part_z = full_z // groups_y
    vmem, smem = pltpu.VMEM, pltpu.SMEM

    lines = exchange(density.reshape(groups_z, slab, size_y, size_z), "gz")
    lines = lines.transpose(1, 2, 0, 3).reshape(slab, size_y, full_z)
    grad_sq = (
        slope_squared(with_halo(lines, ("gx", "gz"), groups_xz, 0), 0)
        + slope_squared(with_halo(lines, "gy", groups_y, 1), 1)
        + slope_squared(jnp.concatenate([lines[..., -2:], lines, lines[..., :2]], axis=2), 2)
    )
    q_zero = saturated_wavevector(lines, grad_sq)
    q_top = global_max(jnp.max(q_zero).reshape(1, 1), ("gz", "gy", "gx"))
    position = jnp.maximum(qpoints - 1.0 + jnp.log(q_zero / q_top) / mesh_step, 0.0)

    rows = slab * size_y
    z_table = hartley(full_z)
    weights = [[float(np.float32(w)) for w in line] for line in spline_matrix(qpoints)]

    def thetas(*refs):
        theta_kernel(qpoints, groups_y, weights, *refs)

    spectra = call(
        thetas,
        (groups_y, qpoints, rows, part_z),
        [vmem] * 4,
        [pltpu.VMEM((qpoints + 2, rows, full_z), jnp.float32), pltpu.VMEM((qpoints * rows, full_z), jnp.float32)],
    )(lines.reshape(rows, full_z), position.reshape(rows, full_z), *split_table(z_table))
    spectra = exchange(spectra, "gy")

    y_table = hartley(full_y).reshape(groups_xz, part_y, groups_y, size_y)
    y_matrix = np.einsum("gkhy,st->gskhty", y_table, np.eye(slab))
    y_matrix = y_matrix.reshape(groups_xz * slab * part_y, groups_y * rows)
    short = slab * part_y
    spectra = call(line_kernel, (groups_xz, qpoints, short, part_z), [vmem] * 3)(*split_table(y_matrix), spectra)
    spectra = exchange(spectra, ("gx", "gz"))

    x_matrix = np.kron(hartley(full_x), np.eye(part_y))
    y_first = lax.axis_index(("gx", "gz")) * part_y
    z_first = lax.axis_index("gy") * part_z
    y_waves = lax.dynamic_slice_in_dim(jnp.asarray(wave_squared(full_y)), y_first, part_y)
    z_waves = lax.dynamic_slice_in_dim(jnp.asarray(wave_squared(full_z)), z_first, part_z)
    x_waves = jnp.asarray(wave_squared(full_x))
    waves = (x_waves[:, None, None] + y_waves[None, :, None] + z_waves[None, None, :]).reshape(-1, part_z)
    levels = jnp.asarray(np.exp(-mesh_step * (2 * qpoints - 2 - np.arange(2 * qpoints - 1))), jnp.float32)
    masses = (range_factor * q_top.reshape(()) * q_top.reshape(())) * levels
    products = call(
        product_kernel,
        spectra.shape,
        [smem, smem, vmem, vmem, vmem, vmem],
        [pltpu.VMEM((qpoints, groups_xz * short, part_z), jnp.float32)],
    )(coupling, masses, *split_table(x_matrix), waves, spectra)
    returned = exchange(products, ("gx", "gz"))

    fields = call(line_kernel, (groups_y, qpoints, rows, part_z), [vmem] * 3)(*split_table(y_matrix.T), returned)
    fields = exchange(fields, "gy")
    scaled = z_table / (full_x * full_y * full_z)
    fields = call(inverse_z_kernel, (groups_z, qpoints, rows, size_z), [vmem] * 3)(*split_table(scaled), fields)
    blocks = exchange(fields, "gz")
    blocks = blocks.reshape(groups_z, qpoints, slab, size_y, size_z)
    return blocks.transpose(1, 0, 2, 3, 4).reshape(qpoints, size_x, size_y, size_z)


def solution(mesh):
    placed = (P("gx", "gy", "gz"), P())
    return jax.shard_map(
        body, mesh=mesh, in_specs=placed, out_specs=P(None, "gx", "gy", "gz"), check_vma=False
    )
```

```python
import math

import jax
import jax.numpy as jnp
import ml_dtypes
import numpy as np
from jax import lax
from jax.experimental import pallas as pl
from jax.experimental.pallas import tpu as pltpu
from jax.sharding import PartitionSpec as P

zab_ratio = 0.8491 / 9.0
q_cut = 5.0
mesh_step = 0.07
range_factor = 1.0
local_weight = 0.25
spline_root = math.sqrt(3.0) - 2.0
vmem_bytes = 60 * 1024 * 1024


def hartley(length):
    ids = np.arange(length)
    angles = 2.0 * np.pi / length * (ids[:, None] * ids[None, :] % length)
    return np.cos(angles) + np.sin(angles)


def split_table(table):
    table = np.asarray(table, np.float32)
    high = table.astype(ml_dtypes.bfloat16)
    low = (table - high.astype(np.float32)).astype(ml_dtypes.bfloat16)
    return jnp.asarray(high), jnp.asarray(low)


def split_value(value):
    high = value.astype(jnp.bfloat16)
    low = (value - high.astype(jnp.float32)).astype(jnp.bfloat16)
    return high, low


def mul(left, right):
    def dot(a, b):
        return jnp.dot(a, b, preferred_element_type=jnp.float32)

    return dot(left[0], right[0]) + (dot(left[0], right[1]) + dot(left[1], right[0]))


def wave_squared(length):
    ids = np.arange(length)
    folded = np.where(2 * ids < length, ids, ids - length)
    wavenum = (2.0 * np.pi / length) * folded
    return (wavenum * wavenum).astype(np.float32)


def spline_matrix(qpoints):
    knots = np.arange(-1, qpoints + 1)
    nodes = np.arange(qpoints)
    return math.sqrt(3.0) * spline_root ** np.abs(knots[None, :] - nodes[:, None]).astype(np.float64)


def saturated_wavevector(density, grad_sq):
    fermi_k = jnp.cbrt(3.0 * math.pi * math.pi * density)
    reduced = grad_sq / (4.0 * fermi_k * fermi_k * density * density)
    raw_q = fermi_k * (1.0 + zab_ratio * reduced)
    scaled = raw_q / q_cut
    powered = scaled
    series = jnp.zeros_like(scaled)
    for term_order in range(1, 13):
        series = series + powered / term_order
        powered = powered * scaled
    return q_cut * (1.0 - jnp.exp(-series))


def with_halo(cells, axis, count, dim):
    size = cells.shape[dim]
    head = lax.slice_in_dim(cells, 0, 2, axis=dim)
    tail = lax.slice_in_dim(cells, size - 2, size, axis=dim)
    before = lax.ppermute(tail, axis, [(i, (i + 1) % count) for i in range(count)])
    after = lax.ppermute(head, axis, [((i + 1) % count, i) for i in range(count)])
    return jnp.concatenate([before, cells, after], axis=dim)


def slope_squared(padded, dim):
    size = padded.shape[dim] - 4

    def at(offset):
        return lax.slice_in_dim(padded, 2 + offset, 2 + offset + size, axis=dim)

    slope = (8.0 * (at(1) - at(-1)) - (at(2) - at(-2))) / 12.0
    return slope * slope


def global_max(value, axes):
    for axis in axes:
        count = lax.axis_size(axis)
        shifted = [
            lax.ppermute(value, axis, [(i, (i + step) % count) for i in range(count)])
            for step in range(1, count)
        ]
        for other in shifted:
            value = jnp.maximum(value, other)
    return value


def theta_kernel(qpoints, weights, dens_ref, pos_ref, high_ref, low_ref, out_ref, spline_ref, theta_ref):
    rows = dens_ref.shape[0]
    position = pos_ref[...]
    for knot in range(qpoints + 2):
        offset = jnp.abs(position - float(knot - 1))
        outer = jnp.maximum(2.0 - offset, 0.0)
        inner = jnp.maximum(1.0 - offset, 0.0)
        spline_ref[knot] = (outer * outer * outer - 4.0 * (inner * inner * inner)) / 6.0

    def build(step, carry):
        first = pl.multiple_of(step * 8, 8)
        picked = pl.ds(first, 8)
        density = dens_ref[picked, :]
        for node in range(qpoints):
            total = weights[node][0] * spline_ref[0, picked, :]
            for knot in range(1, qpoints + 2):
                total = total + weights[node][knot] * spline_ref[knot, picked, :]
            theta_ref[pl.ds(node * rows + first, 8), :] = total * density
        return carry

    lax.fori_loop(0, rows // 8, build, 0)
    table = (high_ref[...], low_ref[...])

    def transform(step, carry):
        chunk = theta_ref[pl.ds(pl.multiple_of(step * 2 * rows, 8), 2 * rows), :]
        product = mul(split_value(chunk), table)
        out_ref[0, pl.ds(2 * step, 2)] = product.reshape(2, rows, product.shape[1])
        return carry

    lax.fori_loop(0, qpoints // 2, transform, 0)


def line_kernel(high_ref, low_ref, in_ref, out_ref):
    groups_in, fields, rows_in, lanes = in_ref.shape
    groups_out, _, rows_out, _ = out_ref.shape
    table = (high_ref[...], low_ref[...])
    for field in range(fields):
        data = in_ref[:, field].reshape(groups_in * rows_in, lanes)
        product = mul(table, split_value(data))
        out_ref[:, field] = product.reshape(groups_out, rows_out, lanes)


def product_kernel(coup_ref, mass_ref, high_ref, low_ref, wave_ref, in_ref, out_ref, spec_ref):
    groups, qpoints, rows, lanes = in_ref.shape
    total_rows = groups * rows
    table = (high_ref[...], low_ref[...])
    for field in range(qpoints):
        data = in_ref[:, field].reshape(total_rows, lanes)
        spec_ref[field] = mul(table, split_value(data))

    def couple(step, carry):
        picked = pl.ds(pl.multiple_of(step * 8, 8), 8)
        waves = wave_ref[picked, :]
        spectra = [spec_ref[field, picked, :] for field in range(qpoints)]
        sums = [None] * qpoints
        for level in range(2 * qpoints - 1):
            mass = mass_ref[level]
            factor = local_weight + mass / (waves + mass)
            for target in range(max(0, level - qpoints + 1), min(qpoints, level + 1)):
                source = level - target
                term = (coup_ref[target, source] * factor) * spectra[source]
                sums[target] = term if sums[target] is None else sums[target] + term
        for field in range(qpoints):
            spec_ref[field, picked, :] = sums[field]
        return carry

    lax.fori_loop(0, total_rows // 8, couple, 0)
    for field in range(qpoints):
        product = mul(table, split_value(spec_ref[field]))
        out_ref[:, field] = product.reshape(groups, rows, lanes)


def inverse_z_kernel(high_ref, low_ref, in_ref, out_ref):
    groups, fields, rows, part = in_ref.shape
    table = (high_ref[...], low_ref[...])

    def transform(step, carry):
        picked = pl.ds(2 * step, 2)
        pieces = [in_ref[group, picked].reshape(2 * rows, part) for group in range(groups)]
        product = mul(split_value(jnp.concatenate(pieces, axis=1)), table)
        groups_out, _, _, part_out = out_ref.shape
        for group in range(groups_out):
            piece = product[:, group * part_out : (group + 1) * part_out]
            out_ref[group, picked] = piece.reshape(2, rows, part_out)
        return carry

    lax.fori_loop(0, fields // 2, transform, 0)


def call(kernel, shape, specs, scratch=()):
    return pl.pallas_call(
        kernel,
        out_shape=jax.ShapeDtypeStruct(shape, jnp.float32),
        in_specs=[pl.BlockSpec(memory_space=space) for space in specs],
        out_specs=pl.BlockSpec(memory_space=pltpu.VMEM),
        scratch_shapes=list(scratch),
        compiler_params=pltpu.CompilerParams(vmem_limit_bytes=vmem_bytes),
    )


def exchange(value, axes):
    return lax.all_to_all(value, axes, split_axis=0, concat_axis=0, tiled=True)


def body(density, coupling):
    size_x, size_y, size_z = density.shape
    qpoints = coupling.shape[0]
    groups_x, groups_y, groups_z = (lax.axis_size("gx"), lax.axis_size("gy"), lax.axis_size("gz"))
    full_x, full_y, full_z = (size_x * groups_x, size_y * groups_y, size_z * groups_z)
    slab = size_x // groups_z
    groups_xz = groups_x * groups_z
    part_y = full_y // groups_xz
    part_z = full_z // groups_y
    vmem, smem = pltpu.VMEM, pltpu.SMEM

    lines = exchange(density.reshape(groups_z, slab, size_y, size_z), "gz")
    lines = lines.transpose(1, 2, 0, 3).reshape(slab, size_y, full_z)
    lines = lax.all_gather(lines, "gy", axis=1, tiled=True)
    grad_sq = (
        slope_squared(with_halo(lines, ("gx", "gz"), groups_xz, 0), 0)
        + slope_squared(jnp.concatenate([lines[:, -2:], lines, lines[:, :2]], axis=1), 1)
        + slope_squared(jnp.concatenate([lines[..., -2:], lines, lines[..., :2]], axis=2), 2)
    )
    q_zero = saturated_wavevector(lines, grad_sq)
    q_top = global_max(jnp.max(q_zero).reshape(1, 1), ("gz", "gx"))
    position = jnp.maximum(qpoints - 1.0 + jnp.log(q_zero / q_top) / mesh_step, 0.0)

    rows = slab * size_y
    plane = slab * full_y
    z_first = lax.axis_index("gy") * part_z
    z_table = hartley(full_z)
    weights = [[float(np.float32(w)) for w in line] for line in spline_matrix(qpoints)]

    def thetas(*refs):
        theta_kernel(qpoints, weights, *refs)

    z_parts = [lax.dynamic_slice_in_dim(t, z_first, part_z, axis=1) for t in split_table(z_table)]
    spectra = call(
        thetas,
        (1, qpoints, plane, part_z),
        [vmem] * 4,
        [pltpu.VMEM((qpoints + 2, plane, full_z), jnp.float32), pltpu.VMEM((qpoints * plane, full_z), jnp.float32)],
    )(lines.reshape(plane, full_z), position.reshape(plane, full_z), *z_parts)

    y_table = hartley(full_y).reshape(groups_xz, part_y, groups_y, size_y)
    y_matrix = np.einsum("gkhy,st->gskhty", y_table, np.eye(slab))
    y_matrix = y_matrix.reshape(groups_xz * slab * part_y, groups_y * rows)
    short = slab * part_y
    y_planes = np.einsum("gky,st->gskty", hartley(full_y).reshape(groups_xz, part_y, full_y), np.eye(slab))
    y_planes = y_planes.reshape(groups_xz * short, plane)
    spectra = call(line_kernel, (groups_xz, qpoints, short, part_z), [vmem] * 3)(*split_table(y_planes), spectra)
    spectra = exchange(spectra, ("gx", "gz"))

    x_matrix = np.kron(hartley(full_x), np.eye(part_y))
    y_first = lax.axis_index(("gx", "gz")) * part_y
    y_waves = lax.dynamic_slice_in_dim(jnp.asarray(wave_squared(full_y)), y_first, part_y)
    z_waves = lax.dynamic_slice_in_dim(jnp.asarray(wave_squared(full_z)), z_first, part_z)
    x_waves = jnp.asarray(wave_squared(full_x))
    waves = (x_waves[:, None, None] + y_waves[None, :, None] + z_waves[None, None, :]).reshape(-1, part_z)
    levels = jnp.asarray(np.exp(-mesh_step * (2 * qpoints - 2 - np.arange(2 * qpoints - 1))), jnp.float32)
    masses = (range_factor * q_top.reshape(()) * q_top.reshape(())) * levels
    products = call(
        product_kernel,
        spectra.shape,
        [smem, smem, vmem, vmem, vmem, vmem],
        [pltpu.VMEM((qpoints, groups_xz * short, part_z), jnp.float32)],
    )(coupling / (full_x * full_y * full_z), masses, *split_table(x_matrix), waves, spectra)
    returned = exchange(products, ("gx", "gz"))

    fields = call(line_kernel, (groups_y, qpoints, rows, part_z), [vmem] * 3)(*split_table(y_matrix.T), returned)
    fields = exchange(fields, "gy")
    fields = call(inverse_z_kernel, (groups_z, qpoints, rows, size_z), [vmem] * 3)(*split_table(z_table), fields)
    blocks = exchange(fields, "gz")
    blocks = blocks.reshape(groups_z, qpoints, slab, size_y, size_z)
    return blocks.transpose(1, 0, 2, 3, 4).reshape(qpoints, size_x, size_y, size_z)


def solution(mesh):
    placed = (P("gx", "gy", "gz"), P())
    return jax.shard_map(
        body, mesh=mesh, in_specs=placed, out_specs=P(None, "gx", "gy", "gz"), check_vma=False
    )
```

```python
import math

import jax
import jax.numpy as jnp
import ml_dtypes
import numpy as np
from jax import lax
from jax.experimental import pallas as pl
from jax.experimental.pallas import tpu as pltpu
from jax.sharding import PartitionSpec as P

zab_ratio = 0.8491 / 9.0
q_cut = 5.0
mesh_step = 0.07
range_factor = 1.0
local_weight = 0.25
spline_root = math.sqrt(3.0) - 2.0
vmem_bytes = 60 * 1024 * 1024


def hartley(length):
    ids = np.arange(length)
    angles = 2.0 * np.pi / length * (ids[:, None] * ids[None, :] % length)
    return np.cos(angles) + np.sin(angles)


def split_table(table):
    table = np.asarray(table, np.float32)
    high = table.astype(ml_dtypes.bfloat16)
    low = (table - high.astype(np.float32)).astype(ml_dtypes.bfloat16)
    return jnp.asarray(high), jnp.asarray(low)


def split_value(value):
    high = value.astype(jnp.bfloat16)
    low = (value - high.astype(jnp.float32)).astype(jnp.bfloat16)
    return high, low


def mul(left, right):
    def dot(a, b):
        return jnp.dot(a, b, preferred_element_type=jnp.float32)

    return dot(left[0], right[0]) + (dot(left[0], right[1]) + dot(left[1], right[0]))


def wave_squared(length):
    ids = np.arange(length)
    folded = np.where(2 * ids < length, ids, ids - length)
    wavenum = (2.0 * np.pi / length) * folded
    return (wavenum * wavenum).astype(np.float32)


def spline_matrix(qpoints):
    knots = np.arange(-1, qpoints + 1)
    nodes = np.arange(qpoints)
    return math.sqrt(3.0) * spline_root ** np.abs(knots[None, :] - nodes[:, None]).astype(np.float64)


def saturated_wavevector(density, grad_sq):
    fermi_k = jnp.cbrt(3.0 * math.pi * math.pi * density)
    reduced = grad_sq / (4.0 * fermi_k * fermi_k * density * density)
    raw_q = fermi_k * (1.0 + zab_ratio * reduced)
    scaled = raw_q / q_cut
    powered = scaled
    series = jnp.zeros_like(scaled)
    for term_order in range(1, 13):
        series = series + powered / term_order
        powered = powered * scaled
    return q_cut * (1.0 - jnp.exp(-series))


def with_halo(cells, axis, count, dim):
    size = cells.shape[dim]
    head = lax.slice_in_dim(cells, 0, 2, axis=dim)
    tail = lax.slice_in_dim(cells, size - 2, size, axis=dim)
    before = lax.ppermute(tail, axis, [(i, (i + 1) % count) for i in range(count)])
    after = lax.ppermute(head, axis, [((i + 1) % count, i) for i in range(count)])
    return jnp.concatenate([before, cells, after], axis=dim)


def slope_squared(padded, dim):
    size = padded.shape[dim] - 4

    def at(offset):
        return lax.slice_in_dim(padded, 2 + offset, 2 + offset + size, axis=dim)

    slope = (8.0 * (at(1) - at(-1)) - (at(2) - at(-2))) / 12.0
    return slope * slope


def global_max(value, axes):
    for axis in axes:
        count = lax.axis_size(axis)
        shifted = [
            lax.ppermute(value, axis, [(i, (i + step) % count) for i in range(count)])
            for step in range(1, count)
        ]
        for other in shifted:
            value = jnp.maximum(value, other)
    return value


def theta_kernel(qpoints, weights, dens_ref, pos_ref, high_ref, low_ref, out_ref, spline_ref, theta_ref):
    rows = dens_ref.shape[0]
    position = pos_ref[...]
    for knot in range(qpoints + 2):
        offset = jnp.abs(position - float(knot - 1))
        outer = jnp.maximum(2.0 - offset, 0.0)
        inner = jnp.maximum(1.0 - offset, 0.0)
        spline_ref[knot] = (outer * outer * outer - 4.0 * (inner * inner * inner)) / 6.0

    def build(step, carry):
        first = pl.multiple_of(step * 8, 8)
        picked = pl.ds(first, 8)
        density = dens_ref[picked, :]
        for node in range(qpoints):
            total = weights[node][0] * spline_ref[0, picked, :]
            for knot in range(1, qpoints + 2):
                total = total + weights[node][knot] * spline_ref[knot, picked, :]
            theta_ref[pl.ds(node * rows + first, 8), :] = total * density
        return carry

    lax.fori_loop(0, rows // 8, build, 0)
    table = (high_ref[...], low_ref[...])

    def transform(step, carry):
        chunk = theta_ref[pl.ds(pl.multiple_of(step * 2 * rows, 8), 2 * rows), :]
        product = mul(split_value(chunk), table)
        out_ref[0, pl.ds(2 * step, 2)] = product.reshape(2, rows, product.shape[1])
        return carry

    lax.fori_loop(0, qpoints // 2, transform, 0)


def line_kernel(high_ref, low_ref, in_ref, out_ref):
    groups_in, fields, rows_in, lanes = in_ref.shape
    groups_out, _, rows_out, _ = out_ref.shape
    table = (high_ref[...], low_ref[...])
    for field in range(fields):
        data = in_ref[:, field].reshape(groups_in * rows_in, lanes)
        product = mul(table, split_value(data))
        out_ref[:, field] = product.reshape(groups_out, rows_out, lanes)


def product_kernel(coup_ref, mass_ref, high_ref, low_ref, wave_ref, in_ref, out_ref, spec_ref):
    groups, qpoints, rows, lanes = in_ref.shape
    total_rows = groups * rows
    table = (high_ref[...], low_ref[...])
    for field in range(qpoints):
        data = in_ref[:, field].reshape(total_rows, lanes)
        spec_ref[field] = mul(table, split_value(data))

    def couple(step, carry):
        picked = pl.ds(pl.multiple_of(step * 8, 8), 8)
        waves = wave_ref[picked, :]
        spectra = [spec_ref[field, picked, :] for field in range(qpoints)]
        sums = [None] * qpoints
        for level in range(2 * qpoints - 1):
            mass = mass_ref[level]
            factor = local_weight + mass / (waves + mass)
            for target in range(max(0, level - qpoints + 1), min(qpoints, level + 1)):
                source = level - target
                term = (coup_ref[target, source] * factor) * spectra[source]
                sums[target] = term if sums[target] is None else sums[target] + term
        for field in range(qpoints):
            spec_ref[field, picked, :] = sums[field]
        return carry

    lax.fori_loop(0, total_rows // 8, couple, 0)
    for field in range(qpoints):
        product = mul(table, split_value(spec_ref[field]))
        out_ref[:, field] = product.reshape(groups, rows, lanes)


def inverse_z_kernel(high_ref, low_ref, in_ref, out_ref):
    groups, fields, rows, part = in_ref.shape
    table = (high_ref[...], low_ref[...])

    def transform(step, carry):
        picked = pl.ds(2 * step, 2)
        pieces = [in_ref[group, picked].reshape(2 * rows, part) for group in range(groups)]
        product = mul(split_value(jnp.concatenate(pieces, axis=1)), table)
        groups_out, _, _, part_out = out_ref.shape
        for group in range(groups_out):
            piece = product[:, group * part_out : (group + 1) * part_out]
            out_ref[group, picked] = piece.reshape(2, rows, part_out)
        return carry

    lax.fori_loop(0, fields // 2, transform, 0)


def call(kernel, shape, specs, scratch=()):
    return pl.pallas_call(
        kernel,
        out_shape=jax.ShapeDtypeStruct(shape, jnp.float32),
        in_specs=[pl.BlockSpec(memory_space=space) for space in specs],
        out_specs=pl.BlockSpec(memory_space=pltpu.VMEM),
        scratch_shapes=list(scratch),
        cost_estimate=pl.CostEstimate(flops=2_000_000_000, bytes_accessed=4_000_000, transcendentals=0),
        compiler_params=pltpu.CompilerParams(vmem_limit_bytes=vmem_bytes),
    )


def exchange(value, axes):
    return lax.all_to_all(value, axes, split_axis=0, concat_axis=0, tiled=True)


def body(density, coupling):
    size_x, size_y, size_z = density.shape
    qpoints = coupling.shape[0]
    groups_x, groups_y, groups_z = (lax.axis_size("gx"), lax.axis_size("gy"), lax.axis_size("gz"))
    full_x, full_y, full_z = (size_x * groups_x, size_y * groups_y, size_z * groups_z)
    slab = size_x // groups_z
    groups_xz = groups_x * groups_z
    part_y = full_y // groups_xz
    part_z = full_z // groups_y
    vmem, smem = pltpu.VMEM, pltpu.SMEM

    lines = exchange(density.reshape(groups_z, slab, size_y, size_z), "gz")
    lines = lines.transpose(1, 2, 0, 3).reshape(slab, size_y, full_z)
    lines = lax.all_gather(lines, "gy", axis=1, tiled=True)
    grad_sq = (
        slope_squared(with_halo(lines, ("gx", "gz"), groups_xz, 0), 0)
        + slope_squared(jnp.concatenate([lines[:, -2:], lines, lines[:, :2]], axis=1), 1)
        + slope_squared(jnp.concatenate([lines[..., -2:], lines, lines[..., :2]], axis=2), 2)
    )
    q_zero = saturated_wavevector(lines, grad_sq)
    q_top = global_max(jnp.max(q_zero).reshape(1, 1), ("gz", "gx"))
    position = jnp.maximum(qpoints - 1.0 + jnp.log(q_zero / q_top) / mesh_step, 0.0)

    rows = slab * size_y
    plane = slab * full_y
    z_first = lax.axis_index("gy") * part_z
    z_table = hartley(full_z)
    weights = [[float(np.float32(w)) for w in line] for line in spline_matrix(qpoints)]

    def thetas(*refs):
        theta_kernel(qpoints, weights, *refs)

    z_parts = [lax.dynamic_slice_in_dim(t, z_first, part_z, axis=1) for t in split_table(z_table)]
    spectra = call(
        thetas,
        (1, qpoints, plane, part_z),
        [vmem] * 4,
        [pltpu.VMEM((qpoints + 2, plane, full_z), jnp.float32), pltpu.VMEM((qpoints * plane, full_z), jnp.float32)],
    )(lines.reshape(plane, full_z), position.reshape(plane, full_z), *z_parts)

    y_table = hartley(full_y).reshape(groups_xz, part_y, groups_y, size_y)
    y_matrix = np.einsum("gkhy,st->gskhty", y_table, np.eye(slab))
    y_matrix = y_matrix.reshape(groups_xz * slab * part_y, groups_y * rows)
    short = slab * part_y
    y_planes = np.einsum("gky,st->gskty", hartley(full_y).reshape(groups_xz, part_y, full_y), np.eye(slab))
    y_planes = y_planes.reshape(groups_xz * short, plane)
    spectra = call(line_kernel, (groups_xz, qpoints, short, part_z), [vmem] * 3)(*split_table(y_planes), spectra)
    spectra = exchange(spectra, ("gx", "gz"))

    x_matrix = np.kron(hartley(full_x), np.eye(part_y))
    y_first = lax.axis_index(("gx", "gz")) * part_y
    y_waves = lax.dynamic_slice_in_dim(jnp.asarray(wave_squared(full_y)), y_first, part_y)
    z_waves = lax.dynamic_slice_in_dim(jnp.asarray(wave_squared(full_z)), z_first, part_z)
    x_waves = jnp.asarray(wave_squared(full_x))
    waves = (x_waves[:, None, None] + y_waves[None, :, None] + z_waves[None, None, :]).reshape(-1, part_z)
    levels = jnp.asarray(np.exp(-mesh_step * (2 * qpoints - 2 - np.arange(2 * qpoints - 1))), jnp.float32)
    masses = (range_factor * q_top.reshape(()) * q_top.reshape(())) * levels
    products = call(
        product_kernel,
        spectra.shape,
        [smem, smem, vmem, vmem, vmem, vmem],
        [pltpu.VMEM((qpoints, groups_xz * short, part_z), jnp.float32)],
    )(coupling / (full_x * full_y * full_z), masses, *split_table(x_matrix), waves, spectra)
    y_back = split_table(y_matrix.T)
    z_back = split_table(z_table)
    middle = qpoints // 4 * 2
    pieces = []
    for part in (products[:, :middle], products[:, middle:]):
        count = part.shape[1]
        part = exchange(part, ("gx", "gz"))
        part = call(line_kernel, (groups_y, count, rows, part_z), [vmem] * 3)(*y_back, part)
        part = exchange(part, "gy")
        part = call(inverse_z_kernel, (groups_z, count, rows, size_z), [vmem] * 3)(*z_back, part)
        part = exchange(part, "gz").reshape(groups_z, count, slab, size_y, size_z)
        pieces.append(part.transpose(1, 0, 2, 3, 4).reshape(count, size_x, size_y, size_z))
    return jnp.concatenate(pieces, axis=0)


def solution(mesh):
    placed = (P("gx", "gy", "gz"), P())
    return jax.shard_map(
        body, mesh=mesh, in_specs=placed, out_specs=P(None, "gx", "gy", "gz"), check_vma=False
    )
```
